128 devices in a mesh: seq: 32 (over z, y, core), tp: 4 (over x).
Axes of the slice: x: 4, y: 4, z: 4, core: 2. Of those that a mesh axis runs over, the one named last changes fastest.
Arguments:
- ssm_inputs: bfloat16 [32768, 8192], P('seq', 'tp'), may hold values from -6 to 6
- step_sizes: float32 [32768, 128], P('seq', 'tp'), as said below
- decay_rates: float32 [128], P('tp'), as said below
- state_inputs: bfloat16 [32768, 128], P('seq'), may hold values from -6 to 6
- state_readout: bfloat16 [32768, 128], P('seq'), may hold values from -0.5 to 0.5
- skip_gain: float32 [128], P('tp'), may hold values from 0.5 to 1.5
- mixed_inputs: bfloat16 [6144, 8192], P('seq', 'tp'), may hold values from -6 to 6
- out_weight: bfloat16 [8192, 8192], P('tp', 'seq'), may hold values from -0.0625 to 0.0625
Outputs:
- ssm_output: bfloat16 [32768, 8192], P('seq', 'tp')
- projected: bfloat16 [6144, 8192], P('seq', 'tp')
The draws below stay inside these ranges and needn't reach their ends.
Inputs may be any that keep to these rules, and one draw needn't show every extreme that they name: `step_sizes`: all entries are positive. `decay_rates`: all entries are positive.
All inputs are finite; a program needn't handle non-finite values.
Results may differ from the reference program's by a relative error of at most 0.017.
Values may be sent and summed in bfloat16 or wider, within the bound.
No kernel may reach another device: no remote copies, remote signals or barrier semaphores. Data moves between devices by JAX's collectives and lax.ppermute only.
A program may use at most 192 MiB of HBM per device.

```python
import math
import jax
import jax.numpy as jnp
from jax import lax

D = 8192
HEADS = 128
HEAD_DIM = 64
STATE = 128
SPAN = 256
SEQLEN = 32768
TOKENS_B = 6144
INNER = 8192
N_TP = 4


def slow_heads(key):
    share = 0.5
    return jax.random.uniform(jax.random.fold_in(key, 11), (HEADS,)) < share


def draw_step_sizes(key, part):
    slow = slow_heads(key)
    length_root = jnp.sqrt(jnp.float32(SEQLEN))
    base = jnp.where(slow, 2.0 / length_root, 0.15)
    first_key, second_key, third_key = jax.random.split(jax.random.fold_in(key, 21), 3)
    coarse = jnp.exp(jax.random.uniform(first_key, (SEQLEN // 512 + 1, HEADS), minval=math.log(0.5), maxval=math.log(2.0)))
    finer = jnp.exp(jax.random.uniform(second_key, (SEQLEN // 32 + 1, HEADS), minval=math.log(0.6), maxval=math.log(1.6)))
    jitter = jax.random.uniform(third_key, (SEQLEN, HEADS), minval=0.7, maxval=1.4)
    position = jnp.arange(SEQLEN)
    return (base[None, :] * coarse[position // 512] * finer[position // 32] * jitter).astype(jnp.float32)


def draw_decay_rates(key, part):
    slow = slow_heads(key)
    length_root = jnp.sqrt(jnp.float32(SEQLEN))
    first_key, second_key = jax.random.split(jax.random.fold_in(key, 31), 2)
    quick = jnp.exp(jax.random.uniform(first_key, (HEADS,), minval=math.log(0.2), maxval=math.log(0.6)))
    lasting = jnp.exp(jax.random.uniform(second_key, (HEADS,), minval=math.log(0.2), maxval=math.log(0.8))) / (2.0 * length_root)
    return jnp.where(slow, lasting, quick).astype(jnp.float32)


def levels(stream_key, extent, shards, smallest, largest):
    def one(axis_at, blocks):
        draws = jax.random.uniform(jax.random.fold_in(jax.random.fold_in(stream_key, 6), axis_at), (blocks,), jnp.float32, smallest / len(shards), largest / len(shards))
        return jnp.repeat(jnp.exp(draws), extent[axis_at] // blocks).reshape((-1,) + (1,) * (len(extent) - axis_at - 1))

    factor_of = one(*shards[0])
    for cut in shards[1:]:
        factor_of = factor_of * one(*cut)
    return factor_of


def scatter_about(stream_key, dims, spread, bound, cuts=(), kind=jnp.bfloat16):
    array = spread * jax.random.normal(stream_key, dims, jnp.float32)
    if cuts:
        array = array * levels(stream_key, dims, cuts, -0.22, 0.18)
    return jnp.clip(array, -bound, bound).astype(kind)


def setup_inputs(seed: int = 0) -> dict:
    keys = jax.random.split(jax.random.key(seed), 9)
    return {
        "ssm_inputs": scatter_about(keys[0], (SEQLEN, INNER), 1.0, 6.0, ((0, 32), (1, 4))),
        "step_sizes": draw_step_sizes(jax.random.fold_in(keys[8], 71), 0),
        "decay_rates": draw_decay_rates(jax.random.fold_in(keys[8], 71), 0),
        "state_inputs": scatter_about(keys[3], (SEQLEN, STATE), 1.0, 6.0, ((0, 32),)),
        "state_readout": scatter_about(keys[4], (SEQLEN, STATE), STATE ** -0.5, 0.5, ((0, 32),)),
        "skip_gain": jnp.clip(1.0 + 0.1 * jax.random.normal(keys[5], (HEADS,), jnp.float32), 0.5, 1.5),
        "mixed_inputs": scatter_about(keys[6], (TOKENS_B, INNER), 1.0, 6.0, ((0, 32), (1, 4))),
        "out_weight": scatter_about(keys[7], (INNER, D), INNER ** -0.5, 0.0625, ((0, 4), (1, 32))),
    }


def round_keep(value):
    return lax.optimization_barrier(value.astype(jnp.bfloat16)).astype(jnp.float32)


def reference(ssm_inputs, step_sizes, decay_rates, state_inputs, state_readout, skip_gain, mixed_inputs, out_weight):
    block_count = SEQLEN // SPAN
    x_blocks = ssm_inputs.reshape(block_count, SPAN, HEADS, HEAD_DIM)
    dt_blocks = step_sizes.reshape(block_count, SPAN, HEADS)
    b_blocks = state_inputs.reshape(block_count, SPAN, STATE)
    c_blocks = state_readout.reshape(block_count, SPAN, STATE)
    lower = jnp.tril(jnp.ones((SPAN, SPAN), dtype=bool))

    def process_block(carried, block):
        x_block, dt_block, b_block, c_block = block
        x_wide = x_block.astype(jnp.float32)
        log_decay = jnp.cumsum(-decay_rates[None, :] * dt_block, axis=0)
        gram = jnp.dot(c_block, b_block.T, preferred_element_type=jnp.float32)
        per_head = log_decay.T
        differ = per_head[:, :, None] - per_head[:, None, :]
        decay = jnp.exp(jnp.where(lower[None], differ, -jnp.inf))
        scores = round_keep(gram[None] * decay * dt_block.T[:, None, :])
        y_diag = jnp.einsum("hts,shp->thp", scores, x_wide)
        entering = round_keep(carried)
        readout = jnp.einsum("tn,hpn->thp", c_block.astype(jnp.float32), entering)
        y_off = jnp.exp(log_decay)[:, :, None] * readout
        output = (y_diag + y_off + skip_gain[None, :, None] * x_wide).astype(jnp.bfloat16)
        tail_weight = jnp.exp(log_decay[-1][None, :] - log_decay) * dt_block
        weighted = round_keep(tail_weight[:, :, None] * x_wide)
        block_state = jnp.einsum("shp,sn->hpn", weighted, b_block.astype(jnp.float32))
        updated = jnp.exp(log_decay[-1])[:, None, None] * carried + block_state
        return updated, output

    start_state = jnp.zeros((HEADS, HEAD_DIM, STATE), jnp.float32)
    final_state, outputs = lax.scan(process_block, start_state, (x_blocks, dt_blocks, b_blocks, c_blocks))
    ssm_output = outputs.reshape(SEQLEN, HEADS * HEAD_DIM)

    group_width = INNER // N_TP

    def add_group(group, total):
        first = (group * group_width)
        columns = lax.dynamic_slice_in_dim(mixed_inputs, first, group_width, 1)
        rows = lax.dynamic_slice_in_dim(out_weight, first, group_width, 0)
        partial_value = jnp.dot(columns, rows, preferred_element_type=jnp.float32)
        return total + round_keep(partial_value)

    summed = lax.fori_loop(0, N_TP, add_group, jnp.zeros((TOKENS_B, D), jnp.float32))
    projected = summed.astype(jnp.bfloat16)
    return ssm_output, projected
```

```python
import functools
import math
import jax
import jax.numpy as jnp
from jax import lax
from jax.experimental import pallas as pl
from jax.experimental.pallas import tpu as pltpu
from jax.sharding import Mesh, PartitionSpec as P

HEAD_DIM = 64
STATE = 128
CHUNK = 128
EXTRA = 8
LOG2E = math.log2(math.e)
F32 = jnp.float32
BF16 = jnp.bfloat16


def split_two(value):
    high = value.astype(BF16)
    low = (value - high.astype(F32)).astype(BF16)
    return high, low


def exact_dot(a, b):
    return lax.dot_general(
        a, b, (((1,), (0,)), ((), ())), precision=lax.Precision.HIGHEST, preferred_element_type=F32
    )


def spread(rows_by_head, one_hot):
    high, low = split_two(rows_by_head)
    both = jnp.concatenate([high, low], axis=1)
    return jnp.dot(both, one_hot, preferred_element_type=F32)


def state_kernel(x_ref, dt_ref, rate_ref, b_ref, hot_ref, out_ref, acc_ref, *, heads):
    step = pl.program_id(0)
    steps = pl.num_programs(0)
    rows = x_ref.shape[0]
    total = dt_ref.shape[1]
    col = lax.broadcasted_iota(jnp.int32, (rows, rows), 0)
    row = lax.broadcasted_iota(jnp.int32, (rows, rows), 1)
    later = (col > row).astype(F32)
    rate = rate_ref[...] * (-LOG2E)
    here = dt_ref[:, pl.ds(pl.multiple_of(step * rows, rows), rows)]
    position = lax.broadcasted_iota(jnp.int32, (heads, total), 1)
    behind = jnp.sum(
        jnp.where(position >= (step + 1) * rows, dt_ref[...], 0.0), axis=1, keepdims=True
    )
    suffix = (exact_dot(here, later) + behind) * rate
    weight = jnp.exp2(suffix) * here
    weight_rows = spread(weight.T, hot_ref[...])
    weighted = (x_ref[...].astype(F32) * weight_rows).astype(BF16)
    term = lax.dot_general(
        b_ref[...], weighted, (((0,), (0,)), ((), ())), preferred_element_type=F32
    )

    @pl.when(step == 0)
    def _():
        acc_ref[...] = term

    @pl.when(step > 0)
    def _():
        acc_ref[...] += term

    @pl.when(step == steps - 1)
    def _():
        whole = jnp.exp2(jnp.sum(dt_ref[...], axis=1, keepdims=True) * rate)
        high, low = split_two(jnp.broadcast_to(whole, (heads, 128)))
        line = lax.broadcasted_iota(jnp.int32, (EXTRA, 128), 0)
        for pair in range(heads // 2):
            flipped = acc_ref[:, pair * 128 : (pair + 1) * 128].T.astype(BF16)
            for k in range(2):
                head = 2 * pair + k
                out_ref[head, :HEAD_DIM, :] = flipped[k * HEAD_DIM : (k + 1) * HEAD_DIM, :]
                out_ref[head, HEAD_DIM:, :] = jnp.where(
                    line < EXTRA // 2,
                    jnp.broadcast_to(high[head : head + 1].astype(F32), (EXTRA, 128)),
                    jnp.broadcast_to(low[head : head + 1].astype(F32), (EXTRA, 128)),
                ).astype(BF16)


def carry_kernel(in_ref, out_ref):
    shards = in_ref.shape[0]

    def one(k, carried):
        out_ref[k] = carried.astype(BF16)
        block = in_ref[k].astype(F32)
        decay = block[HEAD_DIM : HEAD_DIM + 1] + block[HEAD_DIM + EXTRA // 2 : HEAD_DIM + EXTRA // 2 + 1]
        return carried * decay + block[:HEAD_DIM]

    lax.fori_loop(0, shards, one, jnp.zeros((HEAD_DIM, STATE), F32), unroll=4)


def scan_kernel(x_ref, dt_ref, rate_ref, b_ref, c_ref, skip_ref, hot_ref, in_ref, y_ref, s_ref, *, heads):
    step = pl.program_id(0)
    rows = x_ref.shape[0]

    @pl.when(step == 0)
    def _():
        for pair in range(heads // 2):
            both = in_ref[2 * pair : 2 * pair + 2].reshape(128, STATE).astype(F32)
            s_ref[:, pair * 128 : (pair + 1) * 128] = both.T

    t_at = lax.broadcasted_iota(jnp.int32, (rows, rows), 0)
    s_at = lax.broadcasted_iota(jnp.int32, (rows, rows), 1)
    upto = (t_at <= s_at).astype(F32)
    keep = s_at <= t_at
    rate = rate_ref[...] * (-LOG2E)
    dt = dt_ref[...]
    log_rows = exact_dot(dt * rate, upto)
    last = log_rows[:, rows - 1 : rows]
    weight = jnp.exp2(last - log_rows) * dt
    log_source = log_rows - jnp.log2(dt)
    log_cols = log_rows.T
    hot = hot_ref[...]
    grow = spread(jnp.exp2(log_cols), hot)
    weight_rows = spread(weight.T, hot)
    b = b_ref[...]
    c = c_ref[...]
    gram = lax.dot_general(c, b, (((1,), (1,)), ((), ())), preferred_element_type=F32)
    lane = lax.broadcasted_iota(jnp.int32, (rows, 128), 1)
    first_half = lane < HEAD_DIM
    for pair in range(heads // 2):
        cut = slice(pair * 128, (pair + 1) * 128)
        x = x_ref[:, cut]
        x_wide = x.astype(F32)
        state = s_ref[:, cut]
        scores = []
        for k in range(2):
            head = 2 * pair + k
            decay = jnp.exp2(log_cols[:, head : head + 1] - log_source[head : head + 1, :])
            scores.append(jnp.where(keep, gram * decay, 0.0).astype(BF16))
        zero = jnp.zeros_like(x)
        stacked = jnp.concatenate([jnp.where(first_half, x, zero), jnp.where(first_half, zero, x)], axis=0)
        near = jnp.dot(jnp.concatenate(scores, axis=1), stacked, preferred_element_type=F32)
        far = jnp.dot(c, state.astype(BF16), preferred_element_type=F32)
        y = near + grow[:, cut] * far + skip_ref[:, cut] * x_wide
        y_ref[:, cut] = y.astype(BF16)
        weighted = (x_wide * weight_rows[:, cut]).astype(BF16)
        term = lax.dot_general(b, weighted, (((0,), (0,)), ((), ())), preferred_element_type=F32)
        s_ref[:, cut] = state * grow[rows - 1 : rows, cut] + term


def sum_kernel(core_ref, in_ref, out_ref):
    total = in_ref[0, 0].astype(F32)
    for k in range(1, in_ref.shape[0]):
        total = total + in_ref[k, 0].astype(F32)
    total = total.astype(BF16)
    half = total.shape[1] // 2
    own, other = total[:, :half], total[:, half:]
    first = core_ref[0] == 0
    out_ref[:, :half] = jnp.where(first, own, other)
    out_ref[:, half:] = jnp.where(first, other, own)


def shifted(array, axis, by):
    count = lax.axis_size(axis)
    return lax.ppermute(array, axis, [(k, (k + by) % count) for k in range(count)])


def swapped(array):
    return lax.ppermute(array, "c", [(0, 1), (1, 0)])


def ring_gather(array, axis):
    half = array.shape[0] // 2
    behind = shifted(array, axis, 1)
    ahead = shifted(array, axis, -1)
    top = shifted(behind[:half], axis, 1)
    bottom = shifted(ahead[half:], axis, -1)
    return behind, ahead, top, bottom


def per_device(x, step_sizes, decay_rates, b, c, skip_gain, a_own, w_own):
    rows, width = x.shape
    heads = step_sizes.shape[1]
    y_at = lax.axis_index("y")
    z_at = lax.axis_index("z")
    core = lax.axis_index("c")
    dt = step_sizes.T
    rate = decay_rates[:, None]
    one_hot = (jnp.arange(width)[None, :] // HEAD_DIM == jnp.arange(2 * heads)[:, None] % heads).astype(BF16)
    skip = jnp.repeat(skip_gain, HEAD_DIM)[None, :]
    whole = lambda *shape: pl.BlockSpec(shape, lambda i: (0,) * len(shape))

    big = 256
    own_state = pl.pallas_call(
        functools.partial(state_kernel, heads=heads),
        out_shape=jax.ShapeDtypeStruct((heads, HEAD_DIM + EXTRA, STATE), BF16),
        grid=(rows // big,),
        in_specs=[
            pl.BlockSpec((big, width), lambda i: (i, 0)),
            whole(heads, rows),
            whole(heads, 1),
            pl.BlockSpec((big, STATE), lambda i: (i, 0)),
            whole(2 * heads, width),
        ],
        out_specs=whole(heads, HEAD_DIM + EXTRA, STATE),
        scratch_shapes=[pltpu.VMEM((STATE, width), F32)],
        name="state",
    )(x, dt, rate, b, one_hot)

    ring = ("z", "y", "c")
    by_head = lax.all_to_all(own_state, ring, 0, 0, tiled=True)
    carried = pl.pallas_call(
        carry_kernel,
        out_shape=jax.ShapeDtypeStruct((by_head.shape[0], HEAD_DIM, STATE), BF16),
        name="carry",
    )(by_head)
    entering = lax.all_to_all(carried, ring, 0, 0, tiled=True)

    y = pl.pallas_call(
        functools.partial(scan_kernel, heads=heads),
        out_shape=jax.ShapeDtypeStruct((rows, width), BF16),
        grid=(rows // CHUNK,),
        in_specs=[
            pl.BlockSpec((CHUNK, width), lambda i: (i, 0)),
            pl.BlockSpec((heads, CHUNK), lambda i: (0, i)),
            whole(heads, 1),
            pl.BlockSpec((CHUNK, STATE), lambda i: (i, 0)),
            pl.BlockSpec((CHUNK, STATE), lambda i: (i, 0)),
            whole(1, width),
            whole(2 * heads, width),
            whole(heads, HEAD_DIM, STATE),
        ],
        out_specs=pl.BlockSpec((CHUNK, width), lambda i: (i, 0)),
        scratch_shapes=[pltpu.VMEM((STATE, width), F32)],
        name="scan",
    )(x, dt, rate, b, c, skip, one_hot, entering)

    group = lax.axis_size("y")
    a_rows = a_own.shape[0]
    a_behind, a_ahead, a_top, a_bottom = ring_gather(a_own, "y")
    a_all = jnp.zeros((group, a_rows, a_own.shape[1]), BF16)
    put = lambda buf, piece, at: lax.dynamic_update_index_in_dim(buf, piece, at % group, 0)
    a_all = put(a_all, a_own, y_at)
    a_all = put(a_all, a_behind, y_at + group - 1)
    a_all = put(a_all, a_ahead, y_at + 1)
    a_all = put(a_all, jnp.concatenate([a_top, a_bottom], axis=0), y_at + 2)
    a_all = a_all.reshape(group * a_rows, -1)
    w_behind, w_ahead, w_top, w_bottom = ring_gather(w_own, "z")
    partials = jnp.zeros((group, group * a_rows, 2 * w_own.shape[1]), BF16)
    for piece, at in (
        (w_own, z_at),
        (w_behind, z_at + group - 1),
        (w_ahead, z_at + 1),
        (jnp.concatenate([w_top, w_bottom], axis=0), z_at + 2),
    ):
        both = jnp.concatenate([piece, swapped(piece)], axis=1)
        term = jnp.dot(a_all, both, preferred_element_type=F32).astype(BF16)
        partials = put(partials, term, at)
    tiles = partials.reshape(group * group, a_rows, -1)
    got = lax.all_to_all(tiles, ("x", "y"), 0, 0, tiled=True)
    got = got.reshape(group, group, a_rows, -1)
    columns = got.shape[3]
    projected = pl.pallas_call(
        sum_kernel,
        out_shape=jax.ShapeDtypeStruct((a_rows, group * columns), BF16),
        grid_spec=pltpu.PrefetchScalarGridSpec(
            num_scalar_prefetch=1,
            grid=(group,),
            in_specs=[pl.BlockSpec((group, 1, a_rows, columns), lambda i, core: (0, i, 0, 0))],
            out_specs=pl.BlockSpec((a_rows, columns), lambda i, core: (0, i)),
        ),
        name="total",
    )(core[None].astype(jnp.int32), got)
    return y, projected


def solution(mesh):
    chips = (4, 4, 2)
    grid = Mesh(mesh.devices.reshape(*chips, mesh.shape["tp"]), ("z", "y", "c", "x"))
    seq = ("z", "y", "c")
    in_specs = (
        P(seq, "x"),
        P(seq, "x"),
        P("x"),
        P(seq, None),
        P(seq, None),
        P("x"),
        P(seq, "x"),
        P("x", seq),
    )
    out_specs = (P(seq, "x"), P(seq, "x"))
    return jax.shard_map(per_device, mesh=grid, in_specs=in_specs, out_specs=out_specs, check_vma=False)
```
